256 devices in a mesh: seq: 16 (over y_lo, z), tensor: 16 (over y_hi, x, core).
Axes of the slice: x: 4, y: 4 (y_hi: 2, y_lo: 2; y = y_hi * 2 + y_lo), z: 8, core: 2. Of those that a mesh axis runs over, the one named last changes fastest.
Arguments:
- fixed_point: bfloat16 [2048, 4096], P(('seq', 'tensor')), may hold values from -6 to 6
- incoming: bfloat16 [2048, 4096], P(('seq', 'tensor')), may hold values from -6 to 6
- norm_gain: float32 [4096], replicated, may hold values from 0.1 to 1.9
- query_weight: bfloat16 [4096, 4096], P(None, 'tensor'), may hold values from -0.21875 to 0.21875, as said below
- key_weight: bfloat16 [4096, 4096], P(None, 'tensor'), may hold values from -0.265625 to 0.265625, as said below
- value_weight: bfloat16 [4096, 4096], P(None, 'tensor'), may hold values from -0.09375 to 0.09375
- out_weight: bfloat16 [4096, 4096], P('tensor'), may hold values from -0.09375 to 0.09375
- layout: int32 [32, 32], replicated, may hold values 0 or 1
Outputs:
- adjoint: float32 [2048, 4096], P(('seq', 'tensor'))
- gain_grad: float32 [4096], replicated
The draws below stay inside these ranges and needn't reach their ends.
Inputs may be any that keep to these rules, and one draw needn't show every extreme that they name: `query_weight`: entries of the columns of each head are independent; their spread may differ between heads. `key_weight`: entries are independent within a draw; columns of some heads may follow the same head's columns of query_weight. `layout`: A key block strictly before a query block is attended where the entry at row query block, column key block is 1; a block always attends itself causally; entries on or above the diagonal are not read.
All inputs are finite; a program needn't handle non-finite values.
Results may differ from the reference program's by a relative error of at most 0.03.
Values may be sent and summed in bfloat16 or wider, within the bound.
No kernel may reach another device: no remote copies, remote signals or barrier semaphores. Data moves between devices by JAX's collectives and lax.ppermute only.
A program may use at most 64 MiB of HBM per device.

```python
import jax
import jax.numpy as jnp
from jax import lax

D = 4096
HEADS = 32
HEAD_DIM = 128
BLK = 64
ITERS = 2
HEADS_DEV = 2
LENGTH = 2048
NBLK = 32


def projection_pair(key):
    first = jax.random.truncated_normal(jax.random.fold_in(key, 11), -4.0, 4.0, (D, D), jnp.float32)
    second = jax.random.truncated_normal(jax.random.fold_in(key, 23), -4.0, 4.0, (D, D), jnp.float32)
    plain = (2.0 / D) ** 0.5
    query = first * plain
    keyed = second * plain
    return (query, keyed)


def draw_query_weight(key, part):
    return projection_pair(key)[0].astype(jnp.bfloat16)


def draw_key_weight(key, part):
    return projection_pair(key)[1].astype(jnp.bfloat16)


def set_ends(values, stream_key, least, top_value):
    shape = values.shape
    place = [jax.random.randint(jax.random.fold_in(stream_key, axis), (), 0, shape[axis]) for axis in range(len(shape))]
    values = values.at[tuple(place)].set(least)
    longest = shape.index(max(shape))
    place[longest] = (place[longest] + 1) % shape[longest]
    return values.at[tuple(place)].set(top_value)


def block_levels(own_key, shape, cuts, smallest, top_value):
    def one(dim, parts):
        heights = jax.random.uniform(jax.random.fold_in(jax.random.fold_in(own_key, 6), dim), (parts,), jnp.float32, smallest / len(cuts), top_value / len(cuts))
        return jnp.repeat(jnp.exp(heights), shape[dim] // parts).reshape((-1,) + (1,) * (len(shape) - dim - 1))

    loudness = one(*cuts[0])
    for cut in cuts[1:]:
        loudness = loudness * one(*cut)
    return loudness


def noise(stream_key, dims, scale, bound, cuts=(), kind=jnp.bfloat16):
    values = scale * jax.random.normal(stream_key, dims, jnp.float32)
    if cuts:
        values = values * block_levels(stream_key, dims, cuts, -0.22, 0.18)
    return jnp.clip(values, -bound, bound).astype(kind)


def setup_inputs(seed: int = 0) -> dict:
    splits = jax.random.split(jax.random.key(seed), 9)
    fixed_point = noise(splits[0], (LENGTH, D), 1.0, 6.0, ((0, 256),))
    incoming = noise(splits[1], (LENGTH, D), 1.0, 6.0, ((0, 256),))
    norm_gain = jnp.clip(1.0 + 0.18 * jax.random.normal(splits[2], (D,), jnp.float32), 0.1, 1.9)
    query_weight = draw_query_weight(jax.random.fold_in(splits[8], 71), 0)
    key_weight = draw_key_weight(jax.random.fold_in(splits[8], 71), 0)
    value_weight = noise(splits[5], (D, D), D ** -0.5, 0.09375, ((1, 16),))
    out_weight = noise(splits[6], (D, D), D ** -0.5, 0.09375, ((0, 16),))
    layout = set_ends((jax.random.randint(splits[7], (NBLK, NBLK), 0, 4) < 3).astype(jnp.int32), jax.random.fold_in(splits[7], 1), 0, 1)
    return dict(fixed_point=fixed_point, incoming=incoming, norm_gain=norm_gain, query_weight=query_weight, key_weight=key_weight, value_weight=value_weight, out_weight=out_weight, layout=layout)


EPS = 1e-05
THETA = 10000.0
MASKED = -1e+30

def round_low(values):
    return lax.optimization_barrier(values.astype(jnp.bfloat16)).astype(jnp.float32)

def rope_tables(positions):
    freq = THETA ** (-jnp.arange(0, HEAD_DIM, 2, dtype=jnp.float32) / HEAD_DIM)
    angle = positions.astype(jnp.float32)[:, None] * freq[None, :]
    cosine = jnp.concatenate([jnp.cos(angle), jnp.cos(angle)], axis=1)[:, None, :]
    sine = jnp.concatenate([jnp.sin(angle), jnp.sin(angle)], axis=1)[:, None, :]
    return (cosine, sine)

def rotate(values, cosine, sine):
    half = HEAD_DIM // 2
    turned = jnp.concatenate([-values[..., half:], values[..., :half]], axis=-1)
    return values * cosine + turned * sine

def rotate_back(values, cosine, sine):
    half = HEAD_DIM // 2
    weighted = values * sine
    turned = jnp.concatenate([weighted[..., half:], -weighted[..., :half]], axis=-1)
    return values * cosine + turned

def expand_blocks(chosen):
    return jnp.repeat(jnp.repeat(chosen, BLK, axis=0), BLK, axis=1)

def pair_mask(query_pos, key_pos, chosen):
    query_block = (query_pos // BLK)[:, None]
    key_block = (key_pos // BLK)[None, :]
    earlier = (key_block < query_block) & chosen
    same = (key_block == query_block) & (key_pos[None, :] <= query_pos[:, None])
    return earlier | same

def reference(fixed_point, incoming, norm_gain, query_weight, key_weight, value_weight, out_weight, layout):
    groups = HEADS // HEADS_DEV
    width = HEADS_DEV * HEAD_DIM
    score_scale = HEAD_DIM ** (-0.5)
    point = fixed_point.astype(jnp.float32)
    inv_rms = lax.rsqrt(lax.optimization_barrier(jnp.mean(point * point, axis=1, keepdims=True)) + EPS)
    scaled = point * inv_rms
    normed = (norm_gain * scaled).astype(jnp.bfloat16)
    positions = jnp.arange(LENGTH, dtype=jnp.int32)
    cosine, sine = rope_tables(positions)

    def project(weight):
        return jnp.dot(normed, weight, preferred_element_type=jnp.float32).reshape(LENGTH, HEADS, HEAD_DIM)

    def split_heads(values):
        return values.reshape(LENGTH, groups, HEADS_DEV, HEAD_DIM).transpose(1, 0, 2, 3)
    queries = split_heads(rotate(project(query_weight), cosine, sine).astype(jnp.bfloat16))
    keys = split_heads(rotate(project(key_weight), cosine, sine).astype(jnp.bfloat16))
    values = split_heads(project(value_weight).astype(jnp.bfloat16))
    allowed = pair_mask(positions, positions, expand_blocks(layout > 0))[None]

    def probabilities(query_group, key_group):
        scores = jnp.einsum('qhd,khd->hqk', query_group.astype(jnp.float32), key_group.astype(jnp.float32)) * score_scale
        scores = jnp.where(allowed, scores, MASKED)
        return jnp.exp(scores - jax.nn.logsumexp(scores, axis=2, keepdims=True))

    def forward_group(operands):
        query_group, key_group, value_group = operands
        probs = probabilities(query_group, key_group)
        attended = jnp.einsum('hqk,khd->qhd', round_low(probs), value_group.astype(jnp.float32))
        return attended.astype(jnp.bfloat16)
    attended = lax.map(forward_group, (queries, keys, values))
    query_cols = query_weight.reshape(D, groups, width).transpose(1, 0, 2)
    key_cols = key_weight.reshape(D, groups, width).transpose(1, 0, 2)
    value_cols = value_weight.reshape(D, groups, width).transpose(1, 0, 2)
    out_rows = out_weight.reshape(groups, width, D)

    def backprop(cotangent):
        cotangent_low = cotangent.astype(jnp.bfloat16)

        def group_step(total, operands):
            query_group, key_group, value_group, attended_group, query_col, key_col, value_col, out_row = operands
            grad_out = jnp.dot(cotangent_low, out_row.T, preferred_element_type=jnp.float32).astype(jnp.bfloat16)
            grad_wide = grad_out.astype(jnp.float32).reshape(LENGTH, HEADS_DEV, HEAD_DIM)
            delta = lax.optimization_barrier(jnp.sum(grad_wide * attended_group.astype(jnp.float32), axis=2)).T
            probs = probabilities(query_group, key_group)
            grad_probs = jnp.einsum('qhd,khd->hqk', grad_wide, value_group.astype(jnp.float32))
            grad_scores = round_low(probs * (grad_probs - delta[:, :, None]))
            grad_query = jnp.einsum('hqk,khd->qhd', grad_scores, key_group.astype(jnp.float32)) * score_scale
            grad_key = jnp.einsum('hqk,qhd->khd', grad_scores, query_group.astype(jnp.float32)) * score_scale
            grad_value = jnp.einsum('hqk,qhd->khd', round_low(probs), grad_wide)
            query_low = rotate_back(grad_query, cosine, sine).astype(jnp.bfloat16).reshape(LENGTH, width)
            key_low = rotate_back(grad_key, cosine, sine).astype(jnp.bfloat16).reshape(LENGTH, width)
            value_low = grad_value.astype(jnp.bfloat16).reshape(LENGTH, width)
            partial_sum = jnp.dot(query_low, query_col.T, preferred_element_type=jnp.float32)
            partial_sum = partial_sum + jnp.dot(key_low, key_col.T, preferred_element_type=jnp.float32)
            partial_sum = partial_sum + jnp.dot(value_low, value_col.T, preferred_element_type=jnp.float32)
            return (total + round_low(partial_sum), None)
        operands = (queries, keys, values, attended, query_cols, key_cols, value_cols, out_rows)
        grad_normed, _ = lax.scan(group_step, jnp.zeros((LENGTH, D), jnp.float32), operands)
        return grad_normed
    cotangent = incoming.astype(jnp.float32)
    adjoint = cotangent
    gain_total = jnp.zeros((D,), jnp.float32)
    for term_index in range(ITERS):
        grad_normed = backprop(cotangent)
        gain_total = gain_total + lax.optimization_barrier(jnp.sum(grad_normed * scaled, axis=0))
        weighted = norm_gain * grad_normed
        inner = lax.optimization_barrier(jnp.sum(weighted * scaled, axis=1, keepdims=True))
        cotangent = inv_rms * (weighted - scaled * (inner / D))
        adjoint = adjoint + cotangent
    return (adjoint, gain_total * LENGTH ** (-0.5))
```

```python
import functools

import jax
import jax.numpy as jnp
from jax import lax
from jax.experimental import pallas as pl
from jax.experimental.pallas import tpu as pltpu
from jax.sharding import Mesh
from jax.sharding import PartitionSpec as P

HEAD_DIM = 128
BLK = 64
ITERS = 2
YL, Z, YH, X, C = ("seq_0", "seq_1", "tensor_0", "tensor_1", "tensor_2")
TENSOR = (YH, X, C)
SEQ = (YL, Z)
SEQ_TENSOR = (YL, Z, YH, X, C)

EPS = 1e-05
THETA = 10000.0
MASKED = -1e30
SCALE = HEAD_DIM ** (-0.5)
LENGTH = 2048
WIDTH = 4096
CHUNK = 512
STEPS = WIDTH // CHUNK
NT = (((1,), (1,)), ((), ()))
F32 = jnp.float32
BF16 = jnp.bfloat16


def dot(a, b):
    return jnp.dot(a, b, preferred_element_type=F32)


def dot_nt(a, b):
    return lax.dot_general(a, b, NT, preferred_element_type=F32)


def swap(v, axis):
    return lax.ppermute(v, axis, [(0, 1), (1, 0)])


def shift(v, axis, by):
    n = lax.axis_size(axis)
    return lax.ppermute(v, axis, [(i, (i + by) % n) for i in range(n)])


def gather_x_core(rows):
    parts = [rows] + [shift(rows, X, -s) for s in (1, 2, 3)]
    own_core = jnp.concatenate(parts, axis=0)
    return jnp.concatenate([own_core, swap(own_core, C)], axis=0)


def gather_tokens(rows):
    return gather_x_core(jnp.concatenate([rows, swap(rows, YH)], axis=0))


def scatter_core_x(partial):
    half = partial.shape[0] // 2
    low = partial[:half].astype(F32) + swap(partial[half:], C).astype(F32)
    low16 = low.astype(BF16)
    quarter = half // 4
    total = low[:quarter]
    for s in (1, 2, 3):
        total = total + shift(low16[s * quarter : (s + 1) * quarter], X, s).astype(F32)
    return total


def ring_gather(chunk):
    z = lax.axis_index(Z)
    n = lax.axis_size(Z)
    out = jnp.zeros((2, n, *chunk.shape[1:]), chunk.dtype)

    def put(out, v, at, w):
        return lax.dynamic_update_slice(out, v[:, None], (w, at % n, 0, 0))

    out = put(out, chunk, z, 0)
    up = down = chunk
    for j in (1, 2, 3):
        up = shift(up, Z, 1)
        down = shift(down, Z, -1)
        out = put(out, up, z + n - j, 0)
        out = put(out, down, z + j, 0)
    last_low = shift(up[:1], Z, 1)
    last_high = shift(down[1:], Z, -1)
    out = put(out, last_low, z + 4, 0)
    out = put(out, last_high, z + 4, 1)
    return out.reshape(2 * n * chunk.shape[1], chunk.shape[2])


def turned(v):
    return pltpu.roll(v, HEAD_DIM // 2, 1)


def project_kernel(
    flag, fp, inc, gain, wq, wk, wv, wo, cos, sin, perm, own, send, inv_out, acc, square
):
    step = pl.program_id(0)

    @pl.when(step == 0)
    def _():
        acc[...] = jnp.zeros_like(acc)
        square[...] = jnp.zeros_like(square)

    x = fp[...].astype(F32)
    n = (x * gain[...]).astype(BF16)
    acc[:, 0:256] += dot(n, wq[...])
    acc[:, 256:512] += dot(n, wk[...])
    acc[:, 512:768] += dot(n, wv[...])
    acc[:, 768:1024] += dot_nt(inc[...], wo[...])
    x2 = x * x
    square[...] += x2[:, 0:128] + x2[:, 128:256] + x2[:, 256:384] + x2[:, 384:512]

    @pl.when(step == STEPS - 1)
    def _():
        inv = lax.rsqrt(jnp.sum(square[...], axis=1, keepdims=True) * (1.0 / WIDTH) + EPS)
        inv_out[...] = jnp.broadcast_to(inv, inv_out.shape)
        pieces = []
        for h in (0, 1):
            for part in (0, 1, 2, 3):
                v = acc[:, 256 * part + 128 * h : 256 * part + 128 * h + 128]
                if part < 3:
                    v = v * inv
                if part < 2:
                    v = v * cos[...] + turned(v) * sin[...]
                pieces.append(v.astype(BF16))
        both = dot(perm[...], jnp.concatenate(pieces, axis=1)).astype(BF16)

        @pl.when(flag[0] == 0)
        def _():
            own[...] = both[:, :512]
            send[...] = both[:, 512:]

        @pl.when(flag[0] != 0)
        def _():
            own[...] = both[:, 512:]
            send[...] = both[:, :512]


def project(flag, fp, inc, gain, wq, wk, wv, wo, cos, sin, perm):
    rows = fp.shape[0]
    full = lambda shape: pl.BlockSpec(shape, lambda k: (0, 0))
    return pl.pallas_call(
        project_kernel,
        grid=(STEPS,),
        in_specs=[
            pl.BlockSpec(memory_space=pltpu.SMEM),
            pl.BlockSpec((rows, CHUNK), lambda k: (0, k)),
            pl.BlockSpec((rows, CHUNK), lambda k: (0, k)),
            pl.BlockSpec((1, CHUNK), lambda k: (0, k)),
            pl.BlockSpec((CHUNK, 256), lambda k: (k, 0)),
            pl.BlockSpec((CHUNK, 256), lambda k: (k, 0)),
            pl.BlockSpec((CHUNK, 256), lambda k: (k, 0)),
            pl.BlockSpec((256, CHUNK), lambda k: (0, k)),
            full((rows, 128)),
            full((rows, 128)),
            full((rows, rows)),
        ],
        out_specs=[full((rows, 512)), full((rows, 512)), full((rows, 128))],
        out_shape=[
            jax.ShapeDtypeStruct((rows, 512), BF16),
            jax.ShapeDtypeStruct((rows, 512), BF16),
            jax.ShapeDtypeStruct((rows, 128), F32),
        ],
        scratch_shapes=[pltpu.VMEM((rows, 1024), F32), pltpu.VMEM((rows, 128), F32)],
        name="project",
    )(flag, fp, inc, gain, wq, wk, wv, wo, cos, sin, perm)


def as_column(row):
    return jnp.broadcast_to(row, (128, 128)).T


def wide(column):
    return jnp.concatenate([column, column], axis=1)


def own_rows(ref, z, lo, hi):
    return jnp.concatenate(
        [
            ref[pl.ds(pl.multiple_of(z * 128, 128), 128), lo:hi],
            ref[pl.ds(pl.multiple_of(1024 + z * 128, 128), 128), lo:hi],
        ],
        axis=0,
    )


def own_columns(ref, z):
    return wide2(
        as_column(ref[0:1, pl.ds(pl.multiple_of(z * 128, 128), 128)]),
        as_column(ref[0:1, pl.ds(pl.multiple_of(1024 + z * 128, 128), 128)]),
    )


def wide2(a, b):
    return wide(jnp.concatenate([a, b], axis=0))


def backward(z, a, g_ref, g_lo, prow, pcol, ot, delta, cos, sin, d_out):
    gt = g_ref[:, g_lo : g_lo + 128].astype(F32).T
    delta[...] = jnp.sum(gt * ot[...].astype(F32), axis=0, keepdims=True)
    g_own = own_rows(g_ref, z, g_lo, g_lo + 128)
    v_own = own_rows(a, z, 256, 384)
    delta_own = own_columns(delta, z)
    grad_q = jnp.zeros((256, 128), F32)
    grad_k = jnp.zeros((256, 128), F32)
    grad_v = jnp.zeros((256, 128), F32)
    for j in range(8):
        s = slice(256 * j, 256 * j + 256)
        p = prow[:, s].astype(F32)
        ds = (p * (dot_nt(g_own, a[s, 256:384]) - delta_own)).astype(BF16)
        grad_q += dot(ds, a[s, 128:256])
        g = g_ref[s, g_lo : g_lo + 128]
        p16 = pcol[:, s]
        ds = (p16.astype(F32) * (dot_nt(v_own, g) - delta[:, s])).astype(BF16)
        grad_k += dot(ds, a[s, 0:128])
        grad_v += dot(p16, g)
    grad_q = grad_q * SCALE
    grad_k = grad_k * SCALE
    d_out[:, 0:128] = (grad_q * cos[...] - turned(grad_q) * sin[...]).astype(BF16)
    d_out[:, 128:256] = (grad_k * cos[...] - turned(grad_k) * sin[...]).astype(BF16)
    d_out[:, 256:384] = grad_v.astype(BF16)


def first_kernel(
    scal, a, bias, bias_own, tri, cos, sin, d_out, prow, pcol, ot, s_ref, p_ref, lse, delta
):
    z = scal[0]
    vt = a[:, 256:384].astype(F32).T.astype(BF16)
    for i in range(8):
        n = 256 * (i + 1)
        cols = slice(256 * i, n)
        q = a[cols, 0:128]
        peak = jnp.full((8, 256), MASKED, F32)
        for b in range(i + 1):
            s = dot_nt(a[256 * b : 256 * b + 256, 128:256], q) * SCALE
            for r in range(4):
                kb = 4 * b + r
                v = s[64 * r : 64 * r + 64] + bias[kb : kb + 1, cols]
                if b == i:
                    v = v + tri[64 * r : 64 * r + 64, :]
                s_ref[64 * kb : 64 * kb + 64, :] = v
                peak = jnp.maximum(peak, jnp.max(v.reshape(8, 8, 256), axis=0))
        peak = jnp.max(peak, axis=0, keepdims=True)
        total = jnp.zeros((8, 256), F32)
        for kb in range(n // 64):
            p = jnp.exp(s_ref[64 * kb : 64 * kb + 64, :] - peak)
            total = total + jnp.sum(p.reshape(8, 8, 256), axis=0)
            p_ref[64 * kb : 64 * kb + 64, :] = p.astype(BF16)
        total = jnp.sum(total, axis=0, keepdims=True)
        lse[:, cols] = peak + jnp.log(total)
        ot[:, cols] = (dot(vt[:, :n], p_ref[:n, :]) / total).astype(BF16)
    q_own = own_rows(a, z, 0, 128)
    k_own = own_rows(a, z, 128, 256)
    lse_own = own_columns(lse, z)
    row = lax.broadcasted_iota(jnp.int32, (256, 256), 0)
    col = lax.broadcasted_iota(jnp.int32, (256, 256), 1)
    pos = jnp.where(row < 128, row + z * 128, row + (1024 - 128) + z * 128) - col
    for j in range(8):
        s = slice(256 * j, 256 * j + 256)
        k_rows = dot_nt(k_own, a[s, 0:128]) * SCALE - lse[:, s]
        q_rows = dot_nt(q_own, a[s, 128:256]) * SCALE - lse_own
        later_key = jnp.where(pos > 256 * j, MASKED, 0.0)
        later_query = jnp.where(pos < 256 * j, MASKED, 0.0)
        for r in range(4):
            t = slice(64 * r, 64 * r + 64)
            pcol[t, s] = jnp.exp(k_rows[t] + bias_own[r : r + 1, s] + later_key[t]).astype(BF16)
            prow[t, s] = jnp.exp(q_rows[t] + bias_own[4 + r : 5 + r, s] + later_query[t]).astype(
                BF16
            )
    backward(z, a, a, 384, prow, pcol, ot, delta, cos, sin, d_out)


def vmem(count):
    return [pl.BlockSpec(memory_space=pltpu.VMEM)] * count


def first_backward(scal, a, bias, bias_own, tri, cos, sin):
    return pl.pallas_call(
        first_kernel,
        in_specs=[pl.BlockSpec(memory_space=pltpu.SMEM)] + vmem(6),
        out_specs=vmem(4),
        out_shape=[
            jax.ShapeDtypeStruct((256, 384), BF16),
            jax.ShapeDtypeStruct((256, LENGTH), BF16),
            jax.ShapeDtypeStruct((256, LENGTH), BF16),
            jax.ShapeDtypeStruct((128, LENGTH), BF16),
        ],
        scratch_shapes=[
            pltpu.VMEM((LENGTH, 256), F32),
            pltpu.VMEM((LENGTH, 256), BF16),
            pltpu.VMEM((1, LENGTH), F32),
            pltpu.VMEM((1, LENGTH), F32),
        ],
        name="attention_first",
    )(scal, a, bias, bias_own, tri, cos, sin)


def second_kernel(scal, a, g, prow, pcol, ot, cos, sin, d_out, delta):
    backward(scal[0], a, g, 0, prow, pcol, ot, delta, cos, sin, d_out)


def second_backward(scal, a, g, prow, pcol, ot, cos, sin):
    return pl.pallas_call(
        second_kernel,
        in_specs=[pl.BlockSpec(memory_space=pltpu.SMEM)] + vmem(7),
        out_specs=pl.BlockSpec(memory_space=pltpu.VMEM),
        out_shape=jax.ShapeDtypeStruct((256, 384), BF16),
        scratch_shapes=[pltpu.VMEM((1, LENGTH), F32)],
        name="attention_second",
    )(scal, a, g, prow, pcol, ot, cos, sin)


def back_kernel(flag, own, got, perm_t, fp, inv, wq, wk, wv, out, gain_out, d):
    @pl.when(pl.program_id(0) == 0)
    def _():
        first = dot(perm_t[...], own[...]).astype(BF16)
        other = dot(perm_t[...], got[...]).astype(BF16)

        @pl.when(flag[0] == 0)
        def _():
            for part in (0, 1, 2):
                d[:, 256 * part : 256 * part + 128] = first[:, 128 * part : 128 * part + 128]
                d[:, 256 * part + 128 : 256 * part + 256] = other[:, 128 * part : 128 * part + 128]

        @pl.when(flag[0] != 0)
        def _():
            for part in (0, 1, 2):
                d[:, 256 * part : 256 * part + 128] = other[:, 128 * part : 128 * part + 128]
                d[:, 256 * part + 128 : 256 * part + 256] = first[:, 128 * part : 128 * part + 128]

    total = dot_nt(d[:, 0:256], wq[...]) + dot_nt(d[:, 256:512], wk[...])
    total = total + dot_nt(d[:, 512:768], wv[...])
    low = total.astype(BF16)
    out[...] = low
    scale = jnp.concatenate([inv[...]] * (CHUNK // 128), axis=1)
    scaled = fp[...].astype(F32) * scale
    gain_out[...] = jnp.sum(low.astype(F32) * scaled, axis=0, keepdims=True)


def back_project(flag, own, got, perm_t, fp, inv, wq, wk, wv):
    rows = own.shape[0]
    full = lambda shape: pl.BlockSpec(shape, lambda k: (0, 0))
    return pl.pallas_call(
        back_kernel,
        grid=(STEPS,),
        in_specs=[
            pl.BlockSpec(memory_space=pltpu.SMEM),
            full((rows, 384)),
            full((rows, 384)),
            full((rows, rows)),
            pl.BlockSpec((rows, CHUNK), lambda k: (0, k)),
            full((rows, 128)),
            pl.BlockSpec((CHUNK, 256), lambda k: (k, 0)),
            pl.BlockSpec((CHUNK, 256), lambda k: (k, 0)),
            pl.BlockSpec((CHUNK, 256), lambda k: (k, 0)),
        ],
        out_specs=[
            pl.BlockSpec((rows, CHUNK), lambda k: (0, k)),
            pl.BlockSpec((1, CHUNK), lambda k: (0, k)),
        ],
        out_shape=[
            jax.ShapeDtypeStruct((rows, WIDTH), BF16),
            jax.ShapeDtypeStruct((1, WIDTH), F32),
        ],
        scratch_shapes=[pltpu.VMEM((rows, 768), BF16)],
        name="back_project",
    )(flag, own, got, perm_t, fp, inv, wq, wk, wv)


def rope_tables(positions):
    lane = jnp.arange(HEAD_DIM, dtype=jnp.int32)
    half = HEAD_DIM // 2
    freq = THETA ** (-(2 * (lane % half)).astype(F32) / HEAD_DIM)
    angle = positions.astype(F32)[:, None] * freq[None, :]
    sign = jnp.where(lane < half, -1.0, 1.0).astype(F32)
    return jnp.cos(angle), jnp.sin(angle) * sign[None, :]


def chosen_bias(layout):
    count = layout.shape[0]
    row = lax.broadcasted_iota(jnp.int32, (count, count), 0)
    col = lax.broadcasted_iota(jnp.int32, (count, count), 1)
    allowed = ((col < row) & (layout == 1)) | (col == row)
    return jnp.where(allowed, 0.0, MASKED).astype(F32)


def spread(blocks):
    return jnp.repeat(blocks, BLK, axis=1)


def body(
    fixed_point, incoming, norm_gain, query_weight, key_weight, value_weight, out_weight, layout
):
    rows, width = fixed_point.shape
    yl, z, yh, x, c = (lax.axis_index(a) for a in SEQ_TENSOR)
    flag = yl.astype(jnp.int32)[None]
    scal = z.astype(jnp.int32)[None]
    seq_tokens = rows * lax.axis_size(TENSOR)

    i = jnp.arange(seq_tokens, dtype=jnp.int32)
    place = (
        ((i // 8) % 2 ^ yh) * 64 + ((i // 16 + x) % 4) * 16 + ((i // 64) ^ c) * 8 + i % 8
    ).astype(jnp.int32)
    perm = (i[:, None] == place[None, :]).astype(BF16)
    perm_t = (place[:, None] == i[None, :]).astype(BF16)
    first = (yl * 8 + z) * seq_tokens
    cos, sin = rope_tables(first + place)
    own_pos = jnp.concatenate([z * 128 + i, 1024 + z * 128 + i])
    cos_own, sin_own = rope_tables(own_pos)
    blocks = chosen_bias(layout)
    bias_t = spread(blocks.T)
    own_blocks = jnp.concatenate(
        [
            lax.dynamic_slice(blocks.T, (2 * z, 0), (2, 32)),
            lax.dynamic_slice(blocks.T, (16 + 2 * z, 0), (2, 32)),
            lax.dynamic_slice(blocks, (2 * z, 0), (2, 32)),
            lax.dynamic_slice(blocks, (16 + 2 * z, 0), (2, 32)),
        ],
        axis=0,
    )
    bias_own = spread(own_blocks)
    t0 = lax.broadcasted_iota(jnp.int32, (256, 256), 0)
    t1 = lax.broadcasted_iota(jnp.int32, (256, 256), 1)
    tri = jnp.where((t0 // BLK == t1 // BLK) & (t0 > t1), MASKED, 0.0).astype(F32)

    both = gather_tokens(jnp.concatenate([fixed_point, incoming], axis=1))
    fp_all, inc_all = both[:, :width], both[:, width:]
    own, send, inv = project(
        flag,
        fp_all,
        inc_all,
        norm_gain[None, :],
        query_weight,
        key_weight,
        value_weight,
        out_weight,
        cos,
        sin,
        perm,
    )

    def pair_up(own, send):
        got = swap(send, YL)
        lower = jnp.where(yl == 0, own, got)
        upper = jnp.where(yl == 0, got, own)
        return jnp.stack([lower, upper])

    every = ring_gather(pair_up(own, send))
    grads, prow, pcol, ot = first_backward(scal, every, bias_t, bias_own, tri, cos_own, sin_own)

    def partials(grads):
        mine = jnp.where(yl == 0, grads[:seq_tokens], grads[seq_tokens:])
        theirs = jnp.where(yl == 0, grads[seq_tokens:], grads[:seq_tokens])
        got = swap(theirs, YL)
        return back_project(
            flag, mine, got, perm_t, fp_all, inv, query_weight, key_weight, value_weight
        )

    def next_term(grad_normed, scaled, inv_rms):
        weighted = norm_gain * grad_normed
        inner = jnp.sum(weighted * scaled, axis=1, keepdims=True)
        return inv_rms * (weighted - scaled * (inner / width))

    partial, gain_first = partials(grads)
    near = scatter_core_x(partial)
    low = near.astype(BF16)
    got = swap(low, YH).astype(F32)
    near = low.astype(F32) + jnp.concatenate([got[rows:], got[:rows]], axis=0)
    inv_near = inv[: 2 * rows, :1]
    scaled_near = fp_all[: 2 * rows].astype(F32) * inv_near
    term = next_term(near, scaled_near, inv_near)
    adjoint = incoming.astype(F32) + term[:rows]

    terms = gather_x_core(term.astype(BF16))
    grad_out = lax.dot_general(terms, out_weight, NT, preferred_element_type=F32)
    grad_low = dot(perm, grad_out.astype(BF16)).astype(BF16)
    g_own = jnp.where(yl == 0, grad_low[:, :128], grad_low[:, 128:])
    g_send = jnp.where(yl == 0, grad_low[:, 128:], grad_low[:, :128])
    g_every = ring_gather(pair_up(g_own, g_send))
    grads = second_backward(scal, every, g_every, prow, pcol, ot, cos_own, sin_own)

    partial, gain_second = partials(grads)
    near = scatter_core_x(partial)
    low = near[rows:].astype(BF16)
    grad_normed = near[:rows] + swap(low, YH).astype(F32)
    term = next_term(grad_normed, scaled_near[:rows], inv_near[:rows])
    adjoint = adjoint + term

    gain = (gain_first + gain_second).reshape(width // 128, 128)
    gain = gain + swap(gain, C)
    gain = gain + shift(gain, X, 1) + shift(gain, X, 2) + shift(gain, X, 3)
    gain = gain + swap(gain, YH)
    seq_devices = lax.axis_size(SEQ)
    copies = jnp.broadcast_to(gain, (seq_devices, *gain.shape))
    gain = jnp.sum(lax.all_to_all(copies, SEQ, split_axis=0, concat_axis=0, tiled=True), axis=0)
    return (adjoint, gain.reshape(width) * LENGTH ** (-0.5))


def solution(mesh):
    split = Mesh(mesh.devices.reshape(2, 8, 2, 4, 2), SEQ_TENSOR)
    in_specs = (
        P(SEQ_TENSOR, None),
        P(SEQ_TENSOR, None),
        P(),
        P(None, TENSOR),
        P(None, TENSOR),
        P(None, TENSOR),
        P(TENSOR, None),
        P(),
    )
    out_specs = (P(SEQ_TENSOR, None), P())
    return jax.shard_map(body, mesh=split, in_specs=in_specs, out_specs=out_specs, check_vma=False)
```
